32 devices in a mesh: scen: 2 (over x), gx: 16 (over z, y, core).
Axes of the slice: x: 2, y: 2, z: 4, core: 2. Of those that a mesh axis runs over, the one named last changes fastest.
Arguments:
- populations: float32 [54, 16, 4, 8, 256], P('scen', 'gx'), parts along dimension 0, may hold values from 0.15 to 2
- cell_kind: int32 [16, 4, 8, 512], P('gx', None, None, 'scen'), parts along dimension 3, may hold values from 0 to 4, as said below
- profile: int32 [16, 4, 8, 512], P('gx', None, None, 'scen'), parts along dimension 3, may hold values from 0 to 7
- vent_table: float32 [16, 3], P('scen'), parts along dimension 0, may hold values from -0.08 to 0.08
- rates: float32 [27], replicated, may hold values from 1 to 1.9
Outputs:
- advanced: float32 [54, 16, 4, 8, 256], P('scen', 'gx'), parts along dimension 0
The draws below stay inside these ranges and needn't reach their ends.
There are 2 independent parts, one for each index of `scen`. The reference program is written for one: setup_inputs(seed, part) draws one part's arguments, and reference() takes and returns one part's arrays. A program takes and returns all parts, laid end to end along the dimension named above; an argument that names none is the same for every part. Nothing has to cross between parts.
Inputs may be any that keep to these rules, and one draw needn't show every extreme that they name: `cell_kind`: 0 fluid, 1 wall, 2 vent, 3 inflow, 4 outflow.
All inputs are finite; a program needn't handle non-finite values.
Results may differ from the reference program's by a relative error of at most 0.0003.
Values sent between devices are 32-bit elements; how exact they have to be, the bound alone decides.
A program may use at most 64 MiB of HBM per device.

```python
import jax
import jax.numpy as jnp
import numpy as np
from jax import lax

PY = 8
CX = 4
CY = 8
NZ = 256
STEPS = 3
PROFILES = 8
BLOCKS = 16


def draw_populations(key, part):
    first_key, second_key, third_key = jax.random.split(key, 3)
    velocity = jnp.clip(jax.random.normal(first_key, (3, BLOCKS, CX, CY, NZ), jnp.float32) * 0.03, -0.05, 0.05)
    density = 1.0 + jax.random.uniform(third_key, (BLOCKS, CX, CY, NZ), jnp.float32, -0.1, 0.1)
    deviation = jnp.clip(jax.random.normal(second_key, (27, BLOCKS, CX, CY, NZ), jnp.float32) * 0.12, -0.3, 0.3)
    columns = []
    for k in range(27):
        step_x = float(k // 9 - 1)
        step_y = float(k // 3 % 3 - 1)
        step_z = float(k % 3 - 1)
        projected = step_x * velocity[0] + step_y * velocity[1] + step_z * velocity[2]
        columns.append(density * (1.0 + 3.0 * projected))
    return jnp.stack(columns) + deviation


def draw_cell_kind(key, part):
    ticket = jax.random.randint(key, (BLOCKS, CX, CY, NZ), 0, 100)
    return jnp.where(ticket < 70, 0, jnp.where(ticket < 80, 1, jnp.where(ticket < 88, 2, jnp.where(ticket < 94, 3, 4)))).astype(jnp.int32)


def with_ends(drawn, own_key, least, high):
    spot = [jax.random.randint(jax.random.fold_in(own_key, axis), (), 0, length) for axis, length in enumerate(drawn.shape)]
    longest = drawn.shape.index(max(drawn.shape))
    neighbour = spot[:longest] + [(spot[longest] + 1) % drawn.shape[longest]] + spot[longest + 1:]
    return drawn.at[tuple(spot)].set(least).at[tuple(neighbour)].set(high)


def setup_inputs(seed: int = 0, part: int = 0) -> dict:
    key_of = jax.random.split(jax.random.key(seed), 6)
    part_keys = jax.random.split(jax.random.fold_in(key_of[5], part), 6)
    return {
        "populations": draw_populations(jax.random.fold_in(jax.random.fold_in(key_of[5], part), 71), part),
        "cell_kind": draw_cell_kind(jax.random.fold_in(jax.random.fold_in(key_of[5], part), 71), part),
        "profile": with_ends(jax.random.randint(part_keys[2], (BLOCKS, CX, CY, NZ), 0, PROFILES), jax.random.fold_in(part_keys[2], 1), 0, PROFILES - 1).astype(jnp.int32),
        "vent_table": jnp.clip(jax.random.uniform(part_keys[3], (PROFILES, 3), jnp.float32, -0.08, 0.08), -0.08, 0.08),
        "rates": jnp.clip(jax.random.uniform(key_of[4], (27,), jnp.float32, 1.0, 1.9), 1.0, 1.9),
    }


def lattice_tables():
    speeds = np.array([[a - 1.0, b - 1.0, d - 1.0] for a in range(3) for b in range(3) for d in range(3)])
    single = np.array([1.0 / 6.0, 2.0 / 3.0, 1.0 / 6.0])
    weights = np.kron(np.kron(single, single), single)
    powers = np.array([[1.0, 1.0, 1.0], [-1.0, 0.0, 1.0], [1.0, 0.0, 1.0]])
    undo = np.array([[0.0, -0.5, 0.5], [1.0, 0.0, -1.0], [0.0, 0.5, 0.5]])
    moments = np.kron(np.kron(powers, powers), powers)
    inverse = np.kron(np.kron(undo, undo), undo)
    return speeds, weights, moments, inverse


def relax_matrix(rates):
    speeds, weights, moments, inverse = lattice_tables()
    left_part = jnp.asarray(inverse / weights[:, None], jnp.float32) * rates[None, :]
    right_part = jnp.asarray(moments * weights[None, :], jnp.float32)
    return jnp.dot(left_part, right_part, precision=lax.Precision.HIGHEST)


def equilibrium(density, velocity):
    speeds = lattice_tables()[0]
    square = velocity[0] * velocity[0] + velocity[1] * velocity[1] + velocity[2] * velocity[2]
    columns = []
    for k in range(27):
        projected = float(speeds[k, 0]) * velocity[0] + float(speeds[k, 1]) * velocity[1] + float(speeds[k, 2]) * velocity[2]
        columns.append(density * (1.0 + 3.0 * projected + 4.5 * projected * projected - 1.5 * square))
    return jnp.stack(columns)


def macroscopic(scaled):
    speeds, weights, moments, inverse = lattice_tables()
    weight_vec = jnp.asarray(weights, jnp.float32)
    moment_rows = jnp.asarray((weights[:, None] * speeds).T, jnp.float32)
    density = jnp.tensordot(weight_vec, scaled, axes=1, precision=lax.Precision.HIGHEST)
    momentum = jnp.tensordot(moment_rows, scaled, axes=1, precision=lax.Precision.HIGHEST)
    return density, momentum / density[None]


def collide(scaled, matrix):
    density, velocity = macroscopic(scaled)
    layout = scaled.shape
    flattened = (scaled - equilibrium(density, velocity)).reshape(27, -1)
    return scaled - jnp.dot(matrix, flattened, precision=lax.Precision.HIGHEST).reshape(layout)


def profile_velocity(profile, vent_table):
    matches = (profile[None] == jnp.arange(vent_table.shape[0], dtype=jnp.int32)[:, None, None, None]).astype(vent_table.dtype)
    return jnp.tensordot(vent_table.T, matches, axes=1, precision=lax.Precision.HIGHEST)


def finish_pull(collided, shifted_x, types_pad, wall_pad, k):
    speeds = lattice_tables()[0]
    step_x, step_y, step_z = int(speeds[k, 0]), int(speeds[k, 1]), int(speeds[k, 2])
    width_x, width_y, width_z = collided.shape[1], collided.shape[2], collided.shape[3]
    padded = jnp.pad(shifted_x, ((0, 0), (1, 1), (1, 1)))
    source = padded[:, 1 - step_y:1 - step_y + width_y, 1 - step_z:1 - step_z + width_z]
    types_src = types_pad[1 - step_x:1 - step_x + width_x, 1 - step_y:1 - step_y + width_y, 1 - step_z:1 - step_z + width_z]
    wall_src = wall_pad[:, 1 - step_x:1 - step_x + width_x, 1 - step_y:1 - step_y + width_y, 1 - step_z:1 - step_z + width_z]
    projected = float(step_x) * wall_src[0] + float(step_y) * wall_src[1] + float(step_z) * wall_src[2]
    bounce = collided[26 - k] + jnp.where(types_src == 2, 6.0 * projected, 0.0)
    open_cell = (types_src == 0) | (types_src >= 3)
    return jnp.where(open_cell, source, bounce)


def apply_cells(passed, cell_types, cell_speed):
    density, velocity = macroscopic(passed)
    unity = jnp.ones_like(density)
    forced_in = equilibrium(unity, cell_speed)
    forced_out = equilibrium(unity, velocity)
    result = jnp.where(cell_types == 0, passed, 1.0)
    result = jnp.where(cell_types == 3, forced_in, result)
    return jnp.where(cell_types == 4, forced_out, result)


def to_room(blocked):
    blocked = jnp.roll(blocked, PY // 2, axis=blocked.ndim - 4)
    lead = blocked.shape[:-4]
    count, depth, rows, cells = blocked.shape[-4:]
    split = blocked.reshape(lead + (count // PY, PY, depth, rows, cells))
    split = jnp.swapaxes(split, -4, -3)
    return split.reshape(lead + ((count // PY) * depth, PY * rows, cells))


def to_blocks(room, depth, rows):
    lead = room.shape[:-3]
    cells = room.shape[-1]
    split = room.reshape(lead + (room.shape[-3] // depth, depth, PY, rows, cells))
    split = jnp.swapaxes(split, -4, -3)
    blocked = split.reshape(lead + ((room.shape[-3] // depth) * PY, depth, rows, cells))
    return jnp.roll(blocked, -(PY // 2), axis=blocked.ndim - 4)


def reference(populations, cell_kind, profile, vent_table, rates):
    depth, rows = populations.shape[2], populations.shape[3]
    speeds = lattice_tables()[0]
    matrix = relax_matrix(rates)
    room_kind = to_room(cell_kind)
    room_profile = to_room(profile)
    types_pad = jnp.pad(jnp.pad(room_kind, ((1, 1), (0, 0), (0, 0)), mode="wrap"), ((0, 0), (1, 1), (1, 1)), constant_values=1)
    profile_pad = jnp.pad(jnp.pad(room_profile, ((1, 1), (0, 0), (0, 0)), mode="wrap"), ((0, 0), (1, 1), (1, 1)))
    wall_pad = profile_velocity(profile_pad, vent_table)
    cell_speed = wall_pad[:, 1:-1, 1:-1, 1:-1]
    scaled = to_room(populations)
    for iteration in range(STEPS):
        collided = collide(scaled, matrix)
        pulled = []
        for k in range(27):
            shifted_x = jnp.roll(collided[k], int(speeds[k, 0]), axis=0)
            pulled.append(finish_pull(collided, shifted_x, types_pad, wall_pad, k))
        scaled = apply_cells(jnp.stack(pulled), room_kind, cell_speed)
    return to_blocks(scaled, depth, rows)
```

```python
import jax
import jax.numpy as jnp
from jax import lax
from jax.experimental import pallas as pl
from jax.experimental.pallas import tpu as pltpu
from jax.sharding import PartitionSpec as P

PY = 8
STEPS = 3
BIG = 1e30
MESH = pl.DeviceIdType.MESH
VELOCITIES = [(a, b, e) for a in (-1, 0, 1) for b in (-1, 0, 1) for e in (-1, 0, 1)]


def spread(low, mid, high):
    even = low + high
    return even + 4.0 * mid, high - low, even


def gather_back(zeroth, first, second):
    return second - first, zeroth - 0.5 * second, second + first


def along_axes(values, transform):
    values = list(values)
    for stride in (1, 3, 9):
        for start in range(27):
            if (start // stride) % 3 == 0:
                picks = [start, start + stride, start + 2 * stride]
                done = transform(*[values[i] for i in picks])
                for i, value in zip(picks, done):
                    values[i] = value
    return values


def collide(g, rates):
    m = along_axes(g, spread)
    rho, jx, jy, jz = m[0], m[9], m[3], m[1]
    inverse = 1.0 / rho
    u = (jx * inverse, jy * inverse, jz * inverse)
    j = (jx, jy, jz)
    sq = [3.0 * (j[d] * u[d]) for d in range(3)]
    relaxed = []
    for k in range(27):
        powers = (k // 9, k // 3 % 3, k % 3)
        ones = [d for d in range(3) if powers[d] == 1]
        twos = [d for d in range(3) if powers[d] == 2]
        factor = (1.0 / 3.0) ** len(twos)
        scale = 1.0
        for power in powers:
            scale *= 0.25 if power == 0 else 0.5
        rate = rates[k]
        keep = scale - scale * rate
        if len(ones) == 3:
            relaxed.append(keep * m[k])
            continue
        if len(ones) == 0:
            target = rho
            for d in twos:
                target = target + sq[d]
        elif len(ones) == 1:
            target = j[ones[0]]
        else:
            target = j[ones[0]] * u[ones[1]]
        relaxed.append(keep * m[k] + (scale * factor * rate) * target)
    return along_axes(relaxed, gather_back)


def flow_velocity(g):
    s, d = [], []
    for i in range(9):
        low, mid, high = g[3 * i], g[3 * i + 1], g[3 * i + 2]
        s.append(low + high + 4.0 * mid)
        d.append(high - low)
    ss, ds, sd = [], [], []
    for i in range(3):
        low, mid, high = s[3 * i], s[3 * i + 1], s[3 * i + 2]
        ss.append(low + high + 4.0 * mid)
        ds.append(high - low)
        sd.append(d[3 * i] + d[3 * i + 2] + 4.0 * d[3 * i + 1])
    rho = ss[0] + ss[2] + 4.0 * ss[1]
    inverse = 1.0 / rho
    jx = ss[2] - ss[0]
    jy = ds[0] + ds[2] + 4.0 * ds[1]
    jz = sd[0] + sd[2] + 4.0 * sd[1]
    return jx * inverse, jy * inverse, jz * inverse


def along(velocity, c):
    total = None
    for step, part in zip(c, velocity):
        if step:
            part = part if step > 0 else -part
            total = part if total is None else total + part
    return total


def unit_equilibrium(u):
    base = 1.0 - 1.5 * (u[0] * u[0] + u[1] * u[1] + u[2] * u[2])
    out = [None] * 27
    out[13] = base
    for k in range(14, 27):
        p = along(u, VELOCITIES[k])
        even = base + 4.5 * (p * p)
        odd = 3.0 * p
        out[k] = even + odd
        out[26 - k] = even - odd
    return out


def kernel(n, depth, rows, cells, profiles, pops, kinds, profs, table, rates, out,
           gi, kp, kup, kdn, klow, khigh, vs, vlow, vhigh, forced, bounce, c, yup, ydn, ylow, yhigh, ps, og,
           load_sem, ksend, krecv, send, recv, out_sem):
    me = lax.axis_index("gx")
    last = depth - 1

    def dev(offset):
        return {"gx": lax.rem(me + (n + offset), n)}

    row = lax.broadcasted_iota(jnp.int32, (rows, cells), 0)
    lane = lax.broadcasted_iota(jnp.int32, (rows, cells), 1)

    loads = [pltpu.make_async_copy(pops.at[:, 0, p], gi.at[p], load_sem.at[p]) for p in range(depth)]
    load_kind = pltpu.make_async_copy(kinds.at[0], kp.at[0, pl.ds(1, depth)], load_sem.at[depth])
    load_prof = pltpu.make_async_copy(profs.at[0], kp.at[1, pl.ds(1, depth)], load_sem.at[depth + 1])
    order = [0, last] + list(range(1, last))
    for p in order[:2]:
        loads[p].start()
    load_kind.start()
    load_prof.start()
    for p in order[2:]:
        loads[p].start()

    barrier = pltpu.get_barrier_semaphore()
    offsets = (1, -1, PY, -PY, PY + 1, PY - 1, -PY + 1, -PY - 1)
    for offset in offsets:
        pl.semaphore_signal(barrier, inc=1, device_id=dev(offset), device_id_type=MESH)

    def remote(src, dst, s_sem, r_sem, offset):
        return pltpu.make_async_remote_copy(
            src_ref=src, dst_ref=dst, send_sem=s_sem, recv_sem=r_sem,
            device_id=dev(offset), device_id_type=MESH)

    def low_face(s):
        return [
            remote(c.at[s, 1, pl.ds(0, 9)], c.at[s, depth + 1, pl.ds(0, 9)], send.at[s, 0], recv.at[s, 0], -PY),
            remote(yup.at[s, 1, 0], ylow.at[s, depth + 1, 0], send.at[s, 1], recv.at[s, 1], -PY + 1),
            remote(ydn.at[s, 1, 0], yhigh.at[s, depth + 1, 0], send.at[s, 2], recv.at[s, 2], -PY - 1),
        ]

    def high_face(s):
        return [
            remote(c.at[s, depth, pl.ds(18, 9)], c.at[s, 0, pl.ds(18, 9)], send.at[s, 3], recv.at[s, 3], PY),
            remote(yup.at[s, depth, 2], ylow.at[s, 0, 2], send.at[s, 4], recv.at[s, 4], PY + 1),
            remote(ydn.at[s, depth, 2], yhigh.at[s, 0, 2], send.at[s, 5], recv.at[s, 5], PY - 1),
        ]

    def y_rows(s, first, count, base):
        return [
            remote(yup.at[s, pl.ds(first, count)], ylow.at[s, pl.ds(first, count)], send.at[s, base], recv.at[s, base], 1),
            remote(ydn.at[s, pl.ds(first, count)], yhigh.at[s, pl.ds(first, count)], send.at[s, base + 1], recv.at[s, base + 1], -1),
        ]

    def y_low(s):
        return y_rows(s, 1, 1, 6)

    def y_high(s):
        return y_rows(s, depth, 1, 8)

    def y_mid(s):
        return y_rows(s, 2, depth - 2, 10)

    def kind_messages():
        messages = []
        for i, (src, dst, offset) in enumerate((
            (kp.at[:, 1], kp.at[:, depth + 1], -PY),
            (kp.at[:, depth], kp.at[:, 0], PY),
            (kup.at[pl.ds(1, depth)], klow.at[pl.ds(1, depth)], 1),
            (kdn.at[pl.ds(1, depth)], khigh.at[pl.ds(1, depth)], -1),
            (kup.at[1], klow.at[depth + 1], -PY + 1),
            (kdn.at[1], khigh.at[depth + 1], -PY - 1),
            (kup.at[depth], klow.at[0], PY + 1),
            (kdn.at[depth], khigh.at[0], PY - 1),
        )):
            messages.append(remote(src, dst, ksend.at[i], krecv.at[i], offset))
        return messages

    def collide_plane(s, p, values_of):
        for half in range(cells // 128):
            z = slice(half * 128, half * 128 + 128)
            done = collide(values_of(z), rates)
            for k in range(27):
                c[s, p + 1, k, :, z] = done[k]
                a, b, e = k // 9, k // 3 % 3, k % 3
                if b == 2:
                    yup[s, p + 1, a, e, :, z] = done[k][rows - 1:rows, :]
                elif b == 0:
                    ydn[s, p + 1, a, e, :, z] = done[k][0:1, :]

    def first_collide(p):
        collide_plane(0, p, lambda z: [gi[p, k, :, z] for k in range(27)])

    loads[0].wait()
    first_collide(0)
    pl.semaphore_wait(barrier, len(offsets))
    for message in low_face(0) + y_low(0):
        message.start()
    loads[last].wait()
    first_collide(last)
    for message in high_face(0) + y_high(0):
        message.start()
    load_kind.wait()
    load_prof.wait()
    for p in range(1, depth + 1):
        for i in range(2):
            kup[p, i] = kp[i, p, rows - 1:rows, :]
            kdn[p, i] = kp[i, p, 0:1, :]
    for message in kind_messages():
        message.start()
    for p in range(1, last):
        loads[p].wait()

    @pl.loop(1, last)
    def _(p):
        first_collide(p)

    for message in y_mid(0):
        message.start()

    for message in kind_messages():
        message.wait_recv()

    def looked_up(profile):
        parts = [jnp.zeros(profile.shape, jnp.float32) for _ in range(3)]
        for i in range(profiles):
            hit = profile == i
            parts = [jnp.where(hit, table[i, d], parts[d]) for d in range(3)]
        return parts

    def source_terms(kind, profile):
        velocity = looked_up(profile)
        opened = (kind == 0) | (kind >= 3)
        vent = kind == 2
        terms = [jnp.where(vent, 6.0 * part, 0.0) for part in velocity]
        return terms + [jnp.where(opened, 1.0, 0.0)], velocity

    @pl.loop(0, depth + 2)
    def _(pp):
        terms, velocity = source_terms(kp[0, pp], kp[1, pp])
        inflow = kp[0, pp] == 3
        for d in range(4):
            vs[pp, d] = terms[d]
        for d in range(3):
            forced[pp, d] = jnp.where(inflow, velocity[d], 0.0)
        for rows_in, rows_out in ((klow, vlow), (khigh, vhigh)):
            terms, _ = source_terms(rows_in[pp, 0], rows_in[pp, 1])
            for d in range(4):
                rows_out[pp, d] = terms[d]

    def shifted(value, low_row, high_row, b, e):
        if b == 1:
            value = jnp.where(row == 0, low_row(), pltpu.roll(value, 1, 0))
        elif b == -1:
            value = jnp.where(row == rows - 1, high_row(), pltpu.roll(value, rows - 1, 0))
        if e == 1:
            value = pltpu.roll(value, 1, 1)
        elif e == -1:
            value = pltpu.roll(value, cells - 1, 1)
        return value

    place = lax.rem(me + PY // 2, PY)
    below_outside = (row == 0) & (place == 0)
    above_outside = (row == rows - 1) & (place == PY - 1)

    @pl.loop(0, depth)
    def _(p):
        for k, (a, b, e) in enumerate(VELOCITIES):
            pp = p + 1 - a

            def term(ref):
                total = jnp.zeros((1, cells), jnp.float32)
                moved = along([ref[pp, d] for d in range(3)], (a, b, e))
                total = total if moved is None else moved
                return jnp.where(ref[pp, 3] > 0.5, BIG, total)

            value = shifted(term(vs), lambda: term(vlow), lambda: term(vhigh), b, e)
            if b == 1:
                value = jnp.where(below_outside, 0.0, value)
            elif b == -1:
                value = jnp.where(above_outside, 0.0, value)
            if e == 1:
                value = jnp.where(lane == 0, 0.0, value)
            elif e == -1:
                value = jnp.where(lane == cells - 1, 0.0, value)
            bounce[p, k] = value

    def pull_plane(s, p):
        for k, (a, b, e) in enumerate(VELOCITIES):
            pp = p + 1 - a
            value = shifted(
                c[s, pp, k],
                lambda: ylow[s, pp, a + 1, e + 1],
                lambda: yhigh[s, pp, a + 1, e + 1], b, e)
            extra = bounce[p, k]
            ps[k] = jnp.where(extra > 0.5 * BIG, value, c[s, p + 1, 26 - k] + extra)

    def applied(p, z):
        passed = [ps[k, :, z] for k in range(27)]
        kind = kp[0, p + 1, :, z]
        u = flow_velocity(passed)
        outflow = kind == 4
        u = [jnp.where(outflow, u[d], forced[p + 1, d, :, z]) for d in range(3)]
        feq = unit_equilibrium(u)
        fluid = kind == 0
        return [jnp.where(fluid, passed[k], feq[k]) for k in range(27)]

    def update(s, p):
        pull_plane(s, p)
        collide_plane(s + 1, p, lambda z: applied(p, z))

    def finish(s, p):
        pull_plane(s, p)
        for half in range(cells // 128):
            z = slice(half * 128, half * 128 + 128)
            done = applied(p, z)
            for k in range(27):
                og[p, k, :, z] = done[k]

    def store_out(p):
        return pltpu.make_async_copy(og.at[p], out.at[:, 0, p], out_sem.at[p])

    def arrive(messages):
        for message in messages:
            message.wait_recv()

    def begin(messages):
        for message in messages:
            message.start()

    @pl.loop(0, STEPS - 1)
    def _(s):
        arrive(y_low(s) + y_high(s) + y_mid(s))

        @pl.loop(1, last)
        def _(p):
            update(s, p)

        begin(y_mid(s + 1))
        arrive(low_face(s)[1:] + high_face(s)[1:])
        arrive(high_face(s)[:1])
        update(s, 0)
        begin(low_face(s + 1) + y_low(s + 1))
        arrive(low_face(s)[:1])
        update(s, last)
        begin(high_face(s + 1) + y_high(s + 1))

    s = STEPS - 1
    arrive(y_low(s) + y_high(s) + y_mid(s))

    @pl.loop(1, last)
    def _(p):
        finish(s, p)
        store_out(p).start()

    arrive(low_face(s)[1:] + high_face(s)[1:])
    arrive(high_face(s)[:1])
    finish(s, 0)
    store_out(0).start()
    arrive(low_face(s)[:1])
    finish(s, last)
    store_out(last).start()

    for message in kind_messages():
        message.wait_send()
    for s in range(STEPS):
        for message in low_face(s) + high_face(s) + y_low(s) + y_high(s) + y_mid(s):
            message.wait_send()
    for p in range(depth):
        store_out(p).wait()


def solution(mesh):
    n = mesh.shape["gx"]

    def local(populations, cell_kind, profile, vent_table, rates):
        depth, rows, cells = populations.shape[2:]
        profiles = vent_table.shape[0]
        f32, i32 = jnp.float32, jnp.int32
        outer = depth + 2
        vm = pltpu.VMEM
        dma = pltpu.SemaphoreType.DMA

        def body(*refs):
            kernel(n, depth, rows, cells, profiles, *refs)

        return pl.pallas_call(
            body,
            out_shape=jax.ShapeDtypeStruct(populations.shape, f32),
            in_specs=[
                pl.BlockSpec(memory_space=pl.ANY),
                pl.BlockSpec(memory_space=pl.ANY),
                pl.BlockSpec(memory_space=pl.ANY),
                pl.BlockSpec(memory_space=pltpu.SMEM),
                pl.BlockSpec(memory_space=pltpu.SMEM),
            ],
            out_specs=pl.BlockSpec(memory_space=pl.ANY),
            scratch_shapes=[
                vm((depth, 27, rows, cells), f32),
                vm((2, outer, rows, cells), i32),
                vm((outer, 2, 1, cells), i32),
                vm((outer, 2, 1, cells), i32),
                vm((outer, 2, 1, cells), i32),
                vm((outer, 2, 1, cells), i32),
                vm((outer, 4, rows, cells), f32),
                vm((outer, 4, 1, cells), f32),
                vm((outer, 4, 1, cells), f32),
                vm((outer, 3, rows, cells), f32),
                vm((depth, 27, rows, cells), f32),
                vm((STEPS, outer, 27, rows, cells), f32),
                vm((STEPS, outer, 3, 3, 1, cells), f32),
                vm((STEPS, outer, 3, 3, 1, cells), f32),
                vm((STEPS, outer, 3, 3, 1, cells), f32),
                vm((STEPS, outer, 3, 3, 1, cells), f32),
                vm((27, rows, cells), f32),
                vm((depth, 27, rows, cells), f32),
                dma((depth + 2,)),
                dma((8,)),
                dma((8,)),
                dma((STEPS, 12)),
                dma((STEPS, 12)),
                dma((depth,)),
            ],
            compiler_params=pltpu.CompilerParams(collective_id=0, has_side_effects=True),
        )(populations, cell_kind, profile, vent_table, rates)

    return jax.shard_map(
        local,
        mesh=mesh,
        in_specs=(
            P("scen", "gx", None, None, None),
            P("gx", None, None, "scen"),
            P("gx", None, None, "scen"),
            P("scen", None),
            P(),
        ),
        out_specs=P("scen", "gx", None, None, None),
        check_vma=False,
    )
```

```python
import jax
import jax.numpy as jnp
from jax import lax
from jax.experimental import pallas as pl
from jax.experimental.pallas import tpu as pltpu
from jax.sharding import PartitionSpec as P

PY = 8
STEPS = 3
BIG = 1e30
MESH = pl.DeviceIdType.MESH
VELOCITIES = [(a, b, e) for a in (-1, 0, 1) for b in (-1, 0, 1) for e in (-1, 0, 1)]


def spread(low, mid, high):
    even = low + high
    return even + 4.0 * mid, high - low, even


def gather_back(zeroth, first, second):
    return second - first, zeroth - 0.5 * second, second + first


def along_axes(values, transform):
    values = list(values)
    for stride in (1, 3, 9):
        for start in range(27):
            if (start // stride) % 3 == 0:
                picks = [start, start + stride, start + 2 * stride]
                done = transform(*[values[i] for i in picks])
                for i, value in zip(picks, done):
                    values[i] = value
    return values


def collide(g, rates):
    m = along_axes(g, spread)
    rho, jx, jy, jz = m[0], m[9], m[3], m[1]
    inverse = 1.0 / rho
    u = (jx * inverse, jy * inverse, jz * inverse)
    j = (jx, jy, jz)
    sq = [3.0 * (j[d] * u[d]) for d in range(3)]
    relaxed = []
    for k in range(27):
        powers = (k // 9, k // 3 % 3, k % 3)
        ones = [d for d in range(3) if powers[d] == 1]
        twos = [d for d in range(3) if powers[d] == 2]
        factor = (1.0 / 3.0) ** len(twos)
        scale = 1.0
        for power in powers:
            scale *= 0.25 if power == 0 else 0.5
        rate = rates[k]
        keep = scale - scale * rate
        if len(ones) == 3:
            relaxed.append(keep * m[k])
            continue
        if len(ones) == 0:
            target = rho
            for d in twos:
                target = target + sq[d]
        elif len(ones) == 1:
            target = j[ones[0]]
        else:
            target = j[ones[0]] * u[ones[1]]
        relaxed.append(keep * m[k] + (scale * factor * rate) * target)
    return along_axes(relaxed, gather_back)


def flow_velocity(g):
    s, d = [], []
    for i in range(9):
        low, mid, high = g[3 * i], g[3 * i + 1], g[3 * i + 2]
        s.append(low + high + 4.0 * mid)
        d.append(high - low)
    ss, ds, sd = [], [], []
    for i in range(3):
        low, mid, high = s[3 * i], s[3 * i + 1], s[3 * i + 2]
        ss.append(low + high + 4.0 * mid)
        ds.append(high - low)
        sd.append(d[3 * i] + d[3 * i + 2] + 4.0 * d[3 * i + 1])
    rho = ss[0] + ss[2] + 4.0 * ss[1]
    inverse = 1.0 / rho
    jx = ss[2] - ss[0]
    jy = ds[0] + ds[2] + 4.0 * ds[1]
    jz = sd[0] + sd[2] + 4.0 * sd[1]
    return jx * inverse, jy * inverse, jz * inverse


def along(velocity, c):
    total = None
    for step, part in zip(c, velocity):
        if step:
            part = part if step > 0 else -part
            total = part if total is None else total + part
    return total


def unit_equilibrium(u):
    base = 1.0 - 1.5 * (u[0] * u[0] + u[1] * u[1] + u[2] * u[2])
    out = [None] * 27
    out[13] = base
    for k in range(14, 27):
        p = along(u, VELOCITIES[k])
        even = base + 4.5 * (p * p)
        odd = 3.0 * p
        out[k] = even + odd
        out[26 - k] = even - odd
    return out


def kernel(n, depth, rows, cells, profiles, pops, kinds, profs, table_in, rates_in, out,
           table, rates, gi, kp, kup, kdn, klow, khigh, vs, vlow, vhigh, forced, bounce, c, yup, ydn, ylow, yhigh, ps, og,
           load_sem, ksend, krecv, send, recv, out_sem):
    me = lax.axis_index("gx")
    last = depth - 1

    def dev(offset):
        return {"gx": lax.rem(me + (n + offset), n)}

    barrier = pltpu.get_barrier_semaphore()
    offsets = (1, -1, PY, -PY, PY + 1, PY - 1, -PY + 1, -PY - 1)
    for offset in offsets:
        pl.semaphore_signal(barrier, inc=1, device_id=dev(offset), device_id_type=MESH)

    row = lax.broadcasted_iota(jnp.int32, (rows, cells), 0)
    lane = lax.broadcasted_iota(jnp.int32, (rows, cells), 1)

    loads = [pltpu.make_async_copy(pops.at[:, 0, p], gi.at[p], load_sem.at[p]) for p in range(depth)]
    load_kind = pltpu.make_async_copy(kinds.at[0], kp.at[0, pl.ds(1, depth)], load_sem.at[depth])
    load_prof = pltpu.make_async_copy(profs.at[0], kp.at[1, pl.ds(1, depth)], load_sem.at[depth + 1])
    order = [0, last] + list(range(1, last))
    load_rates = pltpu.make_async_copy(rates_in, rates, load_sem.at[depth + 2])
    load_table = pltpu.make_async_copy(table_in, table, load_sem.at[depth + 3])
    load_kind.start()
    load_prof.start()
    load_rates.start()
    load_table.start()
    for p in order:
        loads[p].start()

    def remote(src, dst, s_sem, r_sem, offset):
        return pltpu.make_async_remote_copy(
            src_ref=src, dst_ref=dst, send_sem=s_sem, recv_sem=r_sem,
            device_id=dev(offset), device_id_type=MESH)

    def low_face(s):
        return [
            remote(yup.at[s, 1, 0], ylow.at[s, depth + 1, 0], send.at[s, 1], recv.at[s, 1], -PY + 1),
            remote(ydn.at[s, 1, 0], yhigh.at[s, depth + 1, 0], send.at[s, 2], recv.at[s, 2], -PY - 1),
            remote(c.at[s, 1, pl.ds(0, 3), pl.ds(1, rows - 1)], c.at[s, depth + 1, pl.ds(0, 3), pl.ds(1, rows - 1)], send.at[s, 0], recv.at[s, 0], -PY),
            remote(c.at[s, 1, pl.ds(3, 3)], c.at[s, depth + 1, pl.ds(3, 3)], send.at[s, 12], recv.at[s, 12], -PY),
            remote(c.at[s, 1, pl.ds(6, 3), pl.ds(0, rows - 1)], c.at[s, depth + 1, pl.ds(6, 3), pl.ds(0, rows - 1)], send.at[s, 13], recv.at[s, 13], -PY),
        ]

    def high_face(s):
        return [
            remote(yup.at[s, depth, 2], ylow.at[s, 0, 2], send.at[s, 4], recv.at[s, 4], PY + 1),
            remote(ydn.at[s, depth, 2], yhigh.at[s, 0, 2], send.at[s, 5], recv.at[s, 5], PY - 1),
            remote(c.at[s, depth, pl.ds(18, 3), pl.ds(1, rows - 1)], c.at[s, 0, pl.ds(18, 3), pl.ds(1, rows - 1)], send.at[s, 3], recv.at[s, 3], PY),
            remote(c.at[s, depth, pl.ds(21, 3)], c.at[s, 0, pl.ds(21, 3)], send.at[s, 14], recv.at[s, 14], PY),
            remote(c.at[s, depth, pl.ds(24, 3), pl.ds(0, rows - 1)], c.at[s, 0, pl.ds(24, 3), pl.ds(0, rows - 1)], send.at[s, 15], recv.at[s, 15], PY),
        ]

    def y_rows(s, first, count, base):
        return [
            remote(yup.at[s, pl.ds(first, count)], ylow.at[s, pl.ds(first, count)], send.at[s, base], recv.at[s, base], 1),
            remote(ydn.at[s, pl.ds(first, count)], yhigh.at[s, pl.ds(first, count)], send.at[s, base + 1], recv.at[s, base + 1], -1),
        ]

    def y_low(s):
        return y_rows(s, 1, 1, 6)

    def y_high(s):
        return y_rows(s, depth, 1, 8)

    def y_mid(s):
        return y_rows(s, 2, depth - 2, 10)

    def kind_messages():
        messages = []
        for i, (src, dst, offset) in enumerate((
            (kp.at[:, 1], kp.at[:, depth + 1], -PY),
            (kp.at[:, depth], kp.at[:, 0], PY),
            (kup.at[pl.ds(1, depth)], klow.at[pl.ds(1, depth)], 1),
            (kdn.at[pl.ds(1, depth)], khigh.at[pl.ds(1, depth)], -1),
            (kup.at[1], klow.at[depth + 1], -PY + 1),
            (kdn.at[1], khigh.at[depth + 1], -PY - 1),
            (kup.at[depth], klow.at[0], PY + 1),
            (kdn.at[depth], khigh.at[0], PY - 1),
        )):
            messages.append(remote(src, dst, ksend.at[i], krecv.at[i], offset))
        return messages

    def arrive(messages):
        for message in messages:
            message.wait_recv()

    def begin(messages):
        for message in messages:
            message.start()

    def collide_plane(s, p, values_of):
        for half in range(cells // 128):
            z = slice(half * 128, half * 128 + 128)
            done = collide(values_of(z), rates)
            for k in range(27):
                c[s, p + 1, k, :, z] = done[k]
                a, b, e = k // 9, k // 3 % 3, k % 3
                if b == 2:
                    yup[s, p + 1, a, e, :, z] = done[k][rows - 1:rows, :]
                elif b == 0:
                    ydn[s, p + 1, a, e, :, z] = done[k][0:1, :]

    def first_collide(p):
        collide_plane(0, p, lambda z: [gi[p, k, :, z] for k in range(27)])

    load_kind.wait()
    load_prof.wait()
    for p in range(1, depth + 1):
        for i in range(2):
            kup[p, i] = kp[i, p, rows - 1:rows, :]
            kdn[p, i] = kp[i, p, 0:1, :]
    load_rates.wait()
    load_table.wait()
    loads[0].wait()
    first_collide(0)
    pl.semaphore_wait(barrier, len(offsets))
    begin(kind_messages())
    begin(y_low(0) + low_face(0))
    loads[last].wait()
    first_collide(last)
    begin(y_high(0) + high_face(0))
    for p in range(1, last):
        loads[p].wait()

    @pl.loop(1, last)
    def _(p):
        first_collide(p)

    for message in y_mid(0):
        message.start()

    for message in kind_messages():
        message.wait_recv()

    def looked_up(profile):
        parts = [jnp.zeros(profile.shape, jnp.float32) for _ in range(3)]
        for i in range(profiles):
            hit = profile == i
            parts = [jnp.where(hit, table[d, i], parts[d]) for d in range(3)]
        return parts

    def source_terms(kind, profile):
        velocity = looked_up(profile)
        opened = (kind == 0) | (kind >= 3)
        vent = kind == 2
        terms = [jnp.where(vent, 6.0 * part, 0.0) for part in velocity]
        return terms + [jnp.where(opened, 1.0, 0.0)], velocity

    @pl.loop(0, depth + 2)
    def _(pp):
        terms, velocity = source_terms(kp[0, pp], kp[1, pp])
        inflow = kp[0, pp] == 3
        for d in range(4):
            vs[pp, d] = terms[d]
        for d in range(3):
            forced[pp, d] = jnp.where(inflow, velocity[d], 0.0)
        for rows_in, rows_out in ((klow, vlow), (khigh, vhigh)):
            terms, _ = source_terms(rows_in[pp, 0], rows_in[pp, 1])
            for d in range(4):
                rows_out[pp, d] = terms[d]

    def shifted(value, low_row, high_row, b, e):
        if b == 1:
            value = jnp.where(row == 0, low_row(), pltpu.roll(value, 1, 0))
        elif b == -1:
            value = jnp.where(row == rows - 1, high_row(), pltpu.roll(value, rows - 1, 0))
        if e == 1:
            value = pltpu.roll(value, 1, 1)
        elif e == -1:
            value = pltpu.roll(value, cells - 1, 1)
        return value

    place = lax.rem(me + PY // 2, PY)
    below_outside = (row == 0) & (place == 0)
    above_outside = (row == rows - 1) & (place == PY - 1)

    @pl.loop(0, depth)
    def _(p):
        for k, (a, b, e) in enumerate(VELOCITIES):
            pp = p + 1 - a

            def term(ref):
                total = jnp.zeros((1, cells), jnp.float32)
                moved = along([ref[pp, d] for d in range(3)], (a, b, e))
                total = total if moved is None else moved
                return jnp.where(ref[pp, 3] > 0.5, BIG, total)

            value = shifted(term(vs), lambda: term(vlow), lambda: term(vhigh), b, e)
            if b == 1:
                value = jnp.where(below_outside, 0.0, value)
            elif b == -1:
                value = jnp.where(above_outside, 0.0, value)
            if e == 1:
                value = jnp.where(lane == 0, 0.0, value)
            elif e == -1:
                value = jnp.where(lane == cells - 1, 0.0, value)
            bounce[p, k] = value

    def pull_plane(s, p):
        for k, (a, b, e) in enumerate(VELOCITIES):
            pp = p + 1 - a
            value = shifted(
                c[s, pp, k],
                lambda: ylow[s, pp, a + 1, e + 1],
                lambda: yhigh[s, pp, a + 1, e + 1], b, e)
            extra = bounce[p, k]
            ps[k] = jnp.where(extra > 0.5 * BIG, value, c[s, p + 1, 26 - k] + extra)

    def applied(p, z):
        passed = [ps[k, :, z] for k in range(27)]
        kind = kp[0, p + 1, :, z]
        u = flow_velocity(passed)
        outflow = kind == 4
        u = [jnp.where(outflow, u[d], forced[p + 1, d, :, z]) for d in range(3)]
        feq = unit_equilibrium(u)
        fluid = kind == 0
        return [jnp.where(fluid, passed[k], feq[k]) for k in range(27)]

    def update(s, p):
        pull_plane(s, p)
        collide_plane(s + 1, p, lambda z: applied(p, z))

    def finish(s, p):
        pull_plane(s, p)
        for half in range(cells // 128):
            z = slice(half * 128, half * 128 + 128)
            done = applied(p, z)
            for k in range(27):
                og[p, k, :, z] = done[k]

    def store_out(p):
        return pltpu.make_async_copy(og.at[p], out.at[:, 0, p], out_sem.at[p])

    low = (low_face, y_low, 0, last)
    high = (high_face, y_high, last, 0)
    faces = [low, high]
    for s in range(STEPS):
        arrive(y_low(s) + y_high(s) + y_mid(s))

        @pl.loop(1, last)
        def _(p):
            if s < STEPS - 1:
                update(s, p)
            else:
                finish(s, p)
                store_out(p).start()

        if s < STEPS - 1:
            begin(y_mid(s + 1))
        for face in faces:
            arrive(face[0](s))
            p = face[3]
            if s < STEPS - 1:
                update(s, p)
                leaves = low if p == 0 else high
                begin(leaves[1](s + 1) + leaves[0](s + 1))
            else:
                finish(s, p)
                store_out(p).start()
        faces = faces[::-1]

    for message in kind_messages():
        message.wait_send()
    for s in range(STEPS):
        for message in low_face(s) + high_face(s) + y_low(s) + y_high(s) + y_mid(s):
            message.wait_send()
    for p in range(depth):
        store_out(p).wait()


def solution(mesh):
    n = mesh.shape["gx"]

    def local(populations, cell_kind, profile, vent_table, rates):
        depth, rows, cells = populations.shape[2:]
        profiles = vent_table.shape[0]
        f32, i32 = jnp.float32, jnp.int32
        outer = depth + 2
        vm = pltpu.VMEM
        dma = pltpu.SemaphoreType.DMA

        def body(*refs):
            kernel(n, depth, rows, cells, profiles, *refs)

        return pl.pallas_call(
            body,
            out_shape=jax.ShapeDtypeStruct(populations.shape, f32),
            in_specs=[
                pl.BlockSpec(memory_space=pl.ANY),
                pl.BlockSpec(memory_space=pl.ANY),
                pl.BlockSpec(memory_space=pl.ANY),
                pl.BlockSpec(memory_space=pl.ANY),
                pl.BlockSpec(memory_space=pl.ANY),
            ],
            out_specs=pl.BlockSpec(memory_space=pl.ANY),
            scratch_shapes=[
                pltpu.SMEM((3, profiles), f32),
                pltpu.SMEM((27,), f32),
                vm((depth, 27, rows, cells), f32),
                vm((2, outer, rows, cells), i32),
                vm((outer, 2, 1, cells), i32),
                vm((outer, 2, 1, cells), i32),
                vm((outer, 2, 1, cells), i32),
                vm((outer, 2, 1, cells), i32),
                vm((outer, 4, rows, cells), f32),
                vm((outer, 4, 1, cells), f32),
                vm((outer, 4, 1, cells), f32),
                vm((outer, 3, rows, cells), f32),
                vm((depth, 27, rows, cells), f32),
                vm((STEPS, outer, 27, rows, cells), f32),
                vm((STEPS, outer, 3, 3, 1, cells), f32),
                vm((STEPS, outer, 3, 3, 1, cells), f32),
                vm((STEPS, outer, 3, 3, 1, cells), f32),
                vm((STEPS, outer, 3, 3, 1, cells), f32),
                vm((27, rows, cells), f32),
                vm((depth, 27, rows, cells), f32),
                dma((depth + 4,)),
                dma((8,)),
                dma((8,)),
                dma((STEPS, 16)),
                dma((STEPS, 16)),
                dma((depth,)),
            ],
            compiler_params=pltpu.CompilerParams(collective_id=0, has_side_effects=True),
        )(populations, cell_kind, profile, vent_table.T, rates)

    return jax.shard_map(
        local,
        mesh=mesh,
        in_specs=(
            P("scen", "gx", None, None, None),
            P("gx", None, None, "scen"),
            P("gx", None, None, "scen"),
            P("scen", None),
            P(),
        ),
        out_specs=P("scen", "gx", None, None, None),
        check_vma=False,
    )
```

```python
import jax
import jax.numpy as jnp
from jax import lax
from jax.experimental import pallas as pl
from jax.experimental.pallas import tpu as pltpu
from jax.sharding import PartitionSpec as P

PY = 8
STEPS = 3
BIG = 1e30
MESH = pl.DeviceIdType.MESH
VELOCITIES = [(a, b, e) for a in (-1, 0, 1) for b in (-1, 0, 1) for e in (-1, 0, 1)]


def spread(low, mid, high):
    even = low + high
    return even + 4.0 * mid, high - low, even


def gather_back(zeroth, first, second):
    return second - first, zeroth - 0.5 * second, second + first


def along_axes(values, transform):
    values = list(values)
    for stride in (1, 3, 9):
        for start in range(27):
            if (start // stride) % 3 == 0:
                picks = [start, start + stride, start + 2 * stride]
                done = transform(*[values[i] for i in picks])
                for i, value in zip(picks, done):
                    values[i] = value
    return values


def collide(g, rates):
    m = along_axes(g, spread)
    rho, jx, jy, jz = m[0], m[9], m[3], m[1]
    inverse = 1.0 / rho
    u = (jx * inverse, jy * inverse, jz * inverse)
    j = (jx, jy, jz)
    sq = [3.0 * (j[d] * u[d]) for d in range(3)]
    relaxed = []
    for k in range(27):
        powers = (k // 9, k // 3 % 3, k % 3)
        ones = [d for d in range(3) if powers[d] == 1]
        twos = [d for d in range(3) if powers[d] == 2]
        factor = (1.0 / 3.0) ** len(twos)
        scale = 1.0
        for power in powers:
            scale *= 0.25 if power == 0 else 0.5
        rate = rates[k]
        keep = scale - scale * rate
        if len(ones) == 3:
            relaxed.append(keep * m[k])
            continue
        if len(ones) == 0:
            target = rho
            for d in twos:
                target = target + sq[d]
        elif len(ones) == 1:
            target = j[ones[0]]
        else:
            target = j[ones[0]] * u[ones[1]]
        relaxed.append(keep * m[k] + (scale * factor * rate) * target)
    return along_axes(relaxed, gather_back)


def flow_velocity(g):
    s, d = [], []
    for i in range(9):
        low, mid, high = g[3 * i], g[3 * i + 1], g[3 * i + 2]
        s.append(low + high + 4.0 * mid)
        d.append(high - low)
    ss, ds, sd = [], [], []
    for i in range(3):
        low, mid, high = s[3 * i], s[3 * i + 1], s[3 * i + 2]
        ss.append(low + high + 4.0 * mid)
        ds.append(high - low)
        sd.append(d[3 * i] + d[3 * i + 2] + 4.0 * d[3 * i + 1])
    rho = ss[0] + ss[2] + 4.0 * ss[1]
    inverse = 1.0 / rho
    jx = ss[2] - ss[0]
    jy = ds[0] + ds[2] + 4.0 * ds[1]
    jz = sd[0] + sd[2] + 4.0 * sd[1]
    return jx * inverse, jy * inverse, jz * inverse


def along(velocity, c):
    total = None
    for step, part in zip(c, velocity):
        if step:
            part = part if step > 0 else -part
            total = part if total is None else total + part
    return total


def unit_equilibrium(u):
    base = 1.0 - 1.5 * (u[0] * u[0] + u[1] * u[1] + u[2] * u[2])
    out = [None] * 27
    out[13] = base
    for k in range(14, 27):
        p = along(u, VELOCITIES[k])
        even = base + 4.5 * (p * p)
        odd = 3.0 * p
        out[k] = even + odd
        out[26 - k] = even - odd
    return out


def kernel(n, depth, rows, cells, profiles, pops, kinds, profs, table_in, rates_in, out,
           table, rates, gi, kp, kup, kdn, klow, khigh, vs, vlow, vhigh, forced, bounce, c, yup, ydn, ylow, yhigh, ps,
           load_sem, ksend, krecv, send, recv):
    me = lax.axis_index("gx")
    last = depth - 1

    def dev(offset):
        return {"gx": lax.rem(me + (n + offset), n)}

    barrier = pltpu.get_barrier_semaphore()
    offsets = (1, -1, PY, -PY, PY + 1, PY - 1, -PY + 1, -PY - 1)
    for offset in offsets:
        pl.semaphore_signal(barrier, inc=1, device_id=dev(offset), device_id_type=MESH)

    row = lax.broadcasted_iota(jnp.int32, (rows, cells), 0)
    lane = lax.broadcasted_iota(jnp.int32, (rows, cells), 1)

    loads = [pltpu.make_async_copy(pops.at[:, 0, p], gi.at[p], load_sem.at[p]) for p in range(depth)]
    load_kind = pltpu.make_async_copy(kinds.at[0], kp.at[0, pl.ds(1, depth)], load_sem.at[depth])
    load_prof = pltpu.make_async_copy(profs.at[0], kp.at[1, pl.ds(1, depth)], load_sem.at[depth + 1])
    order = [0, last] + list(range(1, last))
    load_rates = pltpu.make_async_copy(rates_in, rates, load_sem.at[depth + 2])
    load_table = pltpu.make_async_copy(table_in, table, load_sem.at[depth + 3])
    load_kind.start()
    load_prof.start()
    load_rates.start()
    load_table.start()
    for p in order:
        loads[p].start()

    def remote(src, dst, s_sem, r_sem, offset):
        return pltpu.make_async_remote_copy(
            src_ref=src, dst_ref=dst, send_sem=s_sem, recv_sem=r_sem,
            device_id=dev(offset), device_id_type=MESH)

    def low_face(s):
        return [
            remote(yup.at[s, 1, 0], ylow.at[s, depth + 1, 0], send.at[s, 1], recv.at[s, 1], -PY + 1),
            remote(ydn.at[s, 1, 0], yhigh.at[s, depth + 1, 0], send.at[s, 2], recv.at[s, 2], -PY - 1),
            remote(c.at[s, 1, pl.ds(0, 3), pl.ds(1, rows - 1)], c.at[s, depth + 1, pl.ds(0, 3), pl.ds(1, rows - 1)], send.at[s, 0], recv.at[s, 0], -PY),
            remote(c.at[s, 1, pl.ds(3, 3)], c.at[s, depth + 1, pl.ds(3, 3)], send.at[s, 12], recv.at[s, 12], -PY),
            remote(c.at[s, 1, pl.ds(6, 3), pl.ds(0, rows - 1)], c.at[s, depth + 1, pl.ds(6, 3), pl.ds(0, rows - 1)], send.at[s, 13], recv.at[s, 13], -PY),
        ]

    def high_face(s):
        return [
            remote(yup.at[s, depth, 2], ylow.at[s, 0, 2], send.at[s, 4], recv.at[s, 4], PY + 1),
            remote(ydn.at[s, depth, 2], yhigh.at[s, 0, 2], send.at[s, 5], recv.at[s, 5], PY - 1),
            remote(c.at[s, depth, pl.ds(18, 3), pl.ds(1, rows - 1)], c.at[s, 0, pl.ds(18, 3), pl.ds(1, rows - 1)], send.at[s, 3], recv.at[s, 3], PY),
            remote(c.at[s, depth, pl.ds(21, 3)], c.at[s, 0, pl.ds(21, 3)], send.at[s, 14], recv.at[s, 14], PY),
            remote(c.at[s, depth, pl.ds(24, 3), pl.ds(0, rows - 1)], c.at[s, 0, pl.ds(24, 3), pl.ds(0, rows - 1)], send.at[s, 15], recv.at[s, 15], PY),
        ]

    def y_rows(s, planes, dirs, base):
        return [
            remote(yup.at[s, planes, dirs], ylow.at[s, planes, dirs], send.at[s, base], recv.at[s, base], 1),
            remote(ydn.at[s, planes, dirs], yhigh.at[s, planes, dirs], send.at[s, base + 1], recv.at[s, base + 1], -1),
        ]

    def y_low(s):
        return y_rows(s, 1, pl.ds(1, 2), 6)

    def y_high(s):
        return y_rows(s, depth, pl.ds(0, 2), 8)

    def y_mid(s):
        return y_rows(s, pl.ds(2, depth - 2), pl.ds(0, 3), 10)

    def kind_messages():
        messages = []
        for i, (src, dst, offset) in enumerate((
            (kp.at[0, 1], kp.at[0, depth + 1], -PY),
            (kp.at[0, depth], kp.at[0, 0], PY),
            (kup.at[pl.ds(1, depth)], klow.at[pl.ds(1, depth)], 1),
            (kdn.at[pl.ds(1, depth)], khigh.at[pl.ds(1, depth)], -1),
            (kup.at[1, 0], klow.at[depth + 1, 0], -PY + 1),
            (kdn.at[1, 0], khigh.at[depth + 1, 0], -PY - 1),
            (kup.at[depth, 0], klow.at[0, 0], PY + 1),
            (kdn.at[depth, 0], khigh.at[0, 0], PY - 1),
        )):
            messages.append(remote(src, dst, ksend.at[i], krecv.at[i], offset))
        return messages

    def arrive(messages):
        for message in messages:
            message.wait_recv()

    def begin(messages):
        for message in messages:
            message.start()

    def collide_plane(s, p, values_of, adjust=None):
        for half in range(cells // 128):
            z = slice(half * 128, half * 128 + 128)
            done = collide(values_of(z), rates)
            if adjust is not None:
                done = adjust(done, z)
            for k in range(27):
                c[s, p + 1, k, :, z] = done[k]
                a, b, e = k // 9, k // 3 % 3, k % 3
                if b == 2:
                    yup[s, p + 1, a, e, :, z] = done[k][rows - 1:rows, :]
                elif b == 0:
                    ydn[s, p + 1, a, e, :, z] = done[k][0:1, :]

    def first_collide(p, side=None):
        def adjust(done, z):
            solid = vs[p + 1, 3, :, z] < 0.5
            velocity = [vs[p + 1, d, :, z] for d in range(3)]
            done = list(done)
            for k, c_k in enumerate(VELOCITIES):
                if c_k[0] == side:
                    done[k] = jnp.where(solid, along(velocity, c_k), done[k])
            return done

        collide_plane(0, p, lambda z: [gi[p, k, :, z] for k in range(27)],
                      None if side is None else adjust)

    load_kind.wait()
    load_prof.wait()
    for p in range(1, depth + 1):
        for i in range(2):
            kup[p, i] = kp[i, p, rows - 1:rows, :]
            kdn[p, i] = kp[i, p, 0:1, :]
    def looked_up(profile):
        parts = [jnp.zeros(profile.shape, jnp.float32) for _ in range(3)]
        for i in range(profiles):
            hit = profile == i
            parts = [jnp.where(hit, table[d, i], parts[d]) for d in range(3)]
        return parts

    def source_terms(kind, profile):
        velocity = looked_up(profile)
        opened = (kind == 0) | (kind >= 3)
        vent = kind == 2
        terms = [jnp.where(vent, 6.0 * part, 0.0) for part in velocity]
        return terms + [jnp.where(opened, 1.0, 0.0)], velocity

    load_rates.wait()
    load_table.wait()

    @pl.loop(1, depth + 1)
    def _(pp):
        terms, velocity = source_terms(kp[0, pp], kp[1, pp])
        inflow = kp[0, pp] == 3
        for d in range(4):
            vs[pp, d] = terms[d]
        for d in range(3):
            forced[pp, d] = jnp.where(inflow, velocity[d], 0.0)

    loads[0].wait()
    first_collide(0, -1)
    pl.semaphore_wait(barrier, len(offsets))
    begin(kind_messages())
    begin(y_low(0) + low_face(0))
    loads[last].wait()
    first_collide(last, 1)
    begin(y_high(0) + high_face(0))
    for p in range(1, last):
        loads[p].wait()

    @pl.loop(1, last)
    def _(p):
        first_collide(p)

    for message in y_mid(0):
        message.start()

    for message in kind_messages():
        message.wait_recv()

    for pp in (0, depth + 1):
        kind = kp[0, pp]
        vs[pp, 3] = jnp.where((kind == 0) | (kind >= 3), 1.0, 0.0)
        for rows_in, rows_out in ((klow, vlow), (khigh, vhigh)):
            kind = rows_in[pp, 0]
            rows_out[pp, 3] = jnp.where((kind == 0) | (kind >= 3), 1.0, 0.0)

    @pl.loop(1, depth + 1)
    def _(pp):
        for rows_in, rows_out in ((klow, vlow), (khigh, vhigh)):
            terms, _ = source_terms(rows_in[pp, 0], rows_in[pp, 1])
            for d in range(4):
                rows_out[pp, d] = terms[d]

    def shifted(value, low_row, high_row, b, e):
        if b == 1:
            value = jnp.where(row == 0, low_row(), pltpu.roll(value, 1, 0))
        elif b == -1:
            value = jnp.where(row == rows - 1, high_row(), pltpu.roll(value, rows - 1, 0))
        if e == 1:
            value = pltpu.roll(value, 1, 1)
        elif e == -1:
            value = pltpu.roll(value, cells - 1, 1)
        return value

    place = lax.rem(me + PY // 2, PY)
    below_outside = (row == 0) & (place == 0)
    above_outside = (row == rows - 1) & (place == PY - 1)

    def bounce_plane(p, steps_x):
        for k, (a, b, e) in enumerate(VELOCITIES):
            if a not in steps_x:
                continue
            pp = p + 1 - a
            outer = isinstance(pp, int) and pp in (0, depth + 1)

            def term(ref, sent):
                if outer:
                    total = sent
                else:
                    total = along([ref[pp, d] for d in range(3)], (a, b, e))
                    total = jnp.zeros((1, cells), jnp.float32) if total is None else total
                return jnp.where(ref[pp, 3] > 0.5, BIG, total)

            value = shifted(
                term(vs, c[0, pp, k] if outer else None),
                lambda: term(vlow, ylow[0, pp, a + 1, e + 1] if outer else None),
                lambda: term(vhigh, yhigh[0, pp, a + 1, e + 1] if outer else None), b, e)
            if b == 1:
                value = jnp.where(below_outside, 0.0, value)
            elif b == -1:
                value = jnp.where(above_outside, 0.0, value)
            if e == 1:
                value = jnp.where(lane == 0, 0.0, value)
            elif e == -1:
                value = jnp.where(lane == cells - 1, 0.0, value)
            bounce[p, k] = value

    @pl.loop(1, last)
    def _(p):
        bounce_plane(p, (-1, 0, 1))

    bounce_plane(0, (-1, 0))
    bounce_plane(last, (0, 1))

    def pull_plane(s, p):
        for k, (a, b, e) in enumerate(VELOCITIES):
            pp = p + 1 - a
            value = shifted(
                c[s, pp, k],
                lambda: ylow[s, pp, a + 1, e + 1],
                lambda: yhigh[s, pp, a + 1, e + 1], b, e)
            extra = bounce[p, k]
            ps[k] = jnp.where(extra > 0.5 * BIG, value, c[s, p + 1, 26 - k] + extra)

    def applied(p, z):
        passed = [ps[k, :, z] for k in range(27)]
        kind = kp[0, p + 1, :, z]
        u = flow_velocity(passed)
        outflow = kind == 4
        u = [jnp.where(outflow, u[d], forced[p + 1, d, :, z]) for d in range(3)]
        feq = unit_equilibrium(u)
        fluid = kind == 0
        return [jnp.where(fluid, passed[k], feq[k]) for k in range(27)]

    def update(s, p):
        pull_plane(s, p)
        collide_plane(s + 1, p, lambda z: applied(p, z))

    def finish(s, p):
        pull_plane(s, p)
        for half in range(cells // 128):
            z = slice(half * 128, half * 128 + 128)
            done = applied(p, z)
            for k in range(27):
                out[k, 0, p, :, z] = done[k]

    low = (low_face, y_low, 0, last)
    high = (high_face, y_high, last, 0)
    faces = [low, high]
    for s in range(STEPS):
        arrive(y_low(s) + y_high(s) + y_mid(s))

        @pl.loop(1, last)
        def _(p):
            if s < STEPS - 1:
                update(s, p)
            else:
                finish(s, p)

        if s < STEPS - 1:
            begin(y_mid(s + 1))
        for face in faces:
            arrive(face[0](s))
            p = face[3]
            if s == 0:
                bounce_plane(p, (1,) if p == 0 else (-1,))
            if s < STEPS - 1:
                update(s, p)
                leaves = low if p == 0 else high
                begin(leaves[1](s + 1) + leaves[0](s + 1))
            else:
                finish(s, p)
        faces = faces[::-1]

    for message in kind_messages():
        message.wait_send()
    for s in range(STEPS):
        for message in low_face(s) + high_face(s) + y_low(s) + y_high(s) + y_mid(s):
            message.wait_send()


def solution(mesh):
    n = mesh.shape["gx"]

    def local(populations, cell_kind, profile, vent_table, rates):
        depth, rows, cells = populations.shape[2:]
        profiles = vent_table.shape[0]
        f32, i32 = jnp.float32, jnp.int32
        outer = depth + 2
        vm = pltpu.VMEM
        dma = pltpu.SemaphoreType.DMA

        def body(*refs):
            kernel(n, depth, rows, cells, profiles, *refs)

        return pl.pallas_call(
            body,
            out_shape=pltpu.VMEM(populations.shape, f32),
            in_specs=[
                pl.BlockSpec(memory_space=pl.ANY),
                pl.BlockSpec(memory_space=pl.ANY),
                pl.BlockSpec(memory_space=pl.ANY),
                pl.BlockSpec(memory_space=pl.ANY),
                pl.BlockSpec(memory_space=pl.ANY),
            ],
            out_specs=pl.BlockSpec(memory_space=pltpu.VMEM),
            scratch_shapes=[
                pltpu.SMEM((3, profiles), f32),
                pltpu.SMEM((27,), f32),
                vm((depth, 27, rows, cells), f32),
                vm((2, outer, rows, cells), i32),
                vm((outer, 2, 1, cells), i32),
                vm((outer, 2, 1, cells), i32),
                vm((outer, 2, 1, cells), i32),
                vm((outer, 2, 1, cells), i32),
                vm((outer, 4, rows, cells), f32),
                vm((outer, 4, 1, cells), f32),
                vm((outer, 4, 1, cells), f32),
                vm((outer, 3, rows, cells), f32),
                vm((depth, 27, rows, cells), f32),
                vm((STEPS, outer, 27, rows, cells), f32),
                vm((STEPS, outer, 3, 3, 1, cells), f32),
                vm((STEPS, outer, 3, 3, 1, cells), f32),
                vm((STEPS, outer, 3, 3, 1, cells), f32),
                vm((STEPS, outer, 3, 3, 1, cells), f32),
                vm((27, rows, cells), f32),
                dma((depth + 4,)),
                dma((8,)),
                dma((8,)),
                dma((STEPS, 16)),
                dma((STEPS, 16)),
            ],
            compiler_params=pltpu.CompilerParams(collective_id=0, has_side_effects=True, vmem_limit_bytes=32*1024*1024),
        )(*[pltpu.with_memory_space_constraint(x, pltpu.HBM) for x in (populations, cell_kind, profile, vent_table.T, rates)])

    return jax.shard_map(
        local,
        mesh=mesh,
        in_specs=(
            P("scen", "gx", None, None, None),
            P("gx", None, None, "scen"),
            P("gx", None, None, "scen"),
            P("scen", None),
            P(),
        ),
        out_specs=P("scen", "gx", None, None, None),
        check_vma=False,
    )
```

```python
import jax
import jax.numpy as jnp
from jax import lax
from jax.experimental import pallas as pl
from jax.experimental.pallas import tpu as pltpu
from jax.sharding import PartitionSpec as P

PY = 8
STEPS = 3
BIG = 1e30
MESH = pl.DeviceIdType.MESH
VELOCITIES = [(a, b, e) for a in (-1, 0, 1) for b in (-1, 0, 1) for e in (-1, 0, 1)]


def spread(low, mid, high):
    even = low + high
    return even + 4.0 * mid, high - low, even


def gather_back(zeroth, first, second):
    return second - first, zeroth - 0.5 * second, second + first


def along_axes(values, transform):
    values = list(values)
    for stride in (1, 3, 9):
        for start in range(27):
            if (start // stride) % 3 == 0:
                picks = [start, start + stride, start + 2 * stride]
                done = transform(*[values[i] for i in picks])
                for i, value in zip(picks, done):
                    values[i] = value
    return values


def collide(g, rates):
    m = along_axes(g, spread)
    rho, jx, jy, jz = m[0], m[9], m[3], m[1]
    inverse = 1.0 / rho
    u = (jx * inverse, jy * inverse, jz * inverse)
    j = (jx, jy, jz)
    sq = [3.0 * (j[d] * u[d]) for d in range(3)]
    relaxed = []
    for k in range(27):
        powers = (k // 9, k // 3 % 3, k % 3)
        ones = [d for d in range(3) if powers[d] == 1]
        twos = [d for d in range(3) if powers[d] == 2]
        factor = (1.0 / 3.0) ** len(twos)
        scale = 1.0
        for power in powers:
            scale *= 0.25 if power == 0 else 0.5
        rate = rates[k]
        keep = scale - scale * rate
        if len(ones) == 3:
            relaxed.append(keep * m[k])
            continue
        if len(ones) == 0:
            target = rho
            for d in twos:
                target = target + sq[d]
        elif len(ones) == 1:
            target = j[ones[0]]
        else:
            target = j[ones[0]] * u[ones[1]]
        relaxed.append(keep * m[k] + (scale * factor * rate) * target)
    return along_axes(relaxed, gather_back)


def flow_velocity(g):
    s, d = [], []
    for i in range(9):
        low, mid, high = g[3 * i], g[3 * i + 1], g[3 * i + 2]
        s.append(low + high + 4.0 * mid)
        d.append(high - low)
    ss, ds, sd = [], [], []
    for i in range(3):
        low, mid, high = s[3 * i], s[3 * i + 1], s[3 * i + 2]
        ss.append(low + high + 4.0 * mid)
        ds.append(high - low)
        sd.append(d[3 * i] + d[3 * i + 2] + 4.0 * d[3 * i + 1])
    rho = ss[0] + ss[2] + 4.0 * ss[1]
    inverse = 1.0 / rho
    jx = ss[2] - ss[0]
    jy = ds[0] + ds[2] + 4.0 * ds[1]
    jz = sd[0] + sd[2] + 4.0 * sd[1]
    return jx * inverse, jy * inverse, jz * inverse


def along(velocity, c):
    total = None
    for step, part in zip(c, velocity):
        if step:
            part = part if step > 0 else -part
            total = part if total is None else total + part
    return total


def unit_equilibrium(u):
    base = 1.0 - 1.5 * (u[0] * u[0] + u[1] * u[1] + u[2] * u[2])
    out = [None] * 27
    out[13] = base
    for k in range(14, 27):
        p = along(u, VELOCITIES[k])
        even = base + 4.5 * (p * p)
        odd = 3.0 * p
        out[k] = even + odd
        out[26 - k] = even - odd
    return out


def kernel(n, depth, rows, cells, profiles, pops, kinds, profs, table_in, rates_in, out,
           table, rates, gi, kp, kup, kdn, klow, khigh, vs, vlow, vhigh, forced, bounce, c, yup, ydn, ylow, yhigh, ps,
           load_sem, ksend, krecv, send, recv):
    me = lax.axis_index("gx")
    last = depth - 1

    def dev(offset):
        return {"gx": lax.rem(me + (n + offset), n)}

    barrier = pltpu.get_barrier_semaphore()
    offsets = (1, -1, PY, -PY, PY + 1, PY - 1, -PY + 1, -PY - 1)
    for offset in offsets:
        pl.semaphore_signal(barrier, inc=1, device_id=dev(offset), device_id_type=MESH)

    row = lax.broadcasted_iota(jnp.int32, (rows, cells), 0)
    lane = lax.broadcasted_iota(jnp.int32, (rows, cells), 1)

    loads = [pltpu.make_async_copy(pops.at[:, 0, p], gi.at[p], load_sem.at[p]) for p in range(depth)]
    load_kind = pltpu.make_async_copy(kinds.at[0], kp.at[0, pl.ds(1, depth)], load_sem.at[depth])
    load_prof = pltpu.make_async_copy(profs.at[0], kp.at[1, pl.ds(1, depth)], load_sem.at[depth + 1])
    order = [0, last] + list(range(1, last))
    load_rates = pltpu.make_async_copy(rates_in, rates, load_sem.at[depth + 2])
    load_table = pltpu.make_async_copy(table_in, table, load_sem.at[depth + 3])
    load_kind.start()
    load_prof.start()
    load_rates.start()
    load_table.start()
    for p in order:
        loads[p].start()

    def remote(src, dst, s_sem, r_sem, offset):
        return pltpu.make_async_remote_copy(
            src_ref=src, dst_ref=dst, send_sem=s_sem, recv_sem=r_sem,
            device_id=dev(offset), device_id_type=MESH)

    def low_face(s):
        return [
            remote(yup.at[s, 1, 0], ylow.at[s, depth + 1, 0], send.at[s, 1], recv.at[s, 1], -PY + 1),
            remote(ydn.at[s, 1, 0], yhigh.at[s, depth + 1, 0], send.at[s, 2], recv.at[s, 2], -PY - 1),
            remote(c.at[s, 1, pl.ds(0, 3), pl.ds(1, rows - 1)], c.at[s, depth + 1, pl.ds(0, 3), pl.ds(1, rows - 1)], send.at[s, 0], recv.at[s, 0], -PY),
            remote(c.at[s, 1, pl.ds(3, 3)], c.at[s, depth + 1, pl.ds(3, 3)], send.at[s, 12], recv.at[s, 12], -PY),
            remote(c.at[s, 1, pl.ds(6, 3), pl.ds(0, rows - 1)], c.at[s, depth + 1, pl.ds(6, 3), pl.ds(0, rows - 1)], send.at[s, 13], recv.at[s, 13], -PY),
        ]

    def high_face(s):
        return [
            remote(yup.at[s, depth, 2], ylow.at[s, 0, 2], send.at[s, 4], recv.at[s, 4], PY + 1),
            remote(ydn.at[s, depth, 2], yhigh.at[s, 0, 2], send.at[s, 5], recv.at[s, 5], PY - 1),
            remote(c.at[s, depth, pl.ds(18, 3), pl.ds(1, rows - 1)], c.at[s, 0, pl.ds(18, 3), pl.ds(1, rows - 1)], send.at[s, 3], recv.at[s, 3], PY),
            remote(c.at[s, depth, pl.ds(21, 3)], c.at[s, 0, pl.ds(21, 3)], send.at[s, 14], recv.at[s, 14], PY),
            remote(c.at[s, depth, pl.ds(24, 3), pl.ds(0, rows - 1)], c.at[s, 0, pl.ds(24, 3), pl.ds(0, rows - 1)], send.at[s, 15], recv.at[s, 15], PY),
        ]

    def y_rows(s, planes, dirs, base):
        return [
            remote(yup.at[s, planes, dirs], ylow.at[s, planes, dirs], send.at[s, base], recv.at[s, base], 1),
            remote(ydn.at[s, planes, dirs], yhigh.at[s, planes, dirs], send.at[s, base + 1], recv.at[s, base + 1], -1),
        ]

    def y_low(s):
        return y_rows(s, 1, pl.ds(1, 2), 6)

    def y_high(s):
        return y_rows(s, depth, pl.ds(0, 2), 8)

    def y_mid(s):
        return y_rows(s, pl.ds(2, depth - 2), pl.ds(0, 3), 10)

    def kind_messages():
        messages = []
        for i, (src, dst, offset) in enumerate((
            (kp.at[0, 1], kp.at[0, depth + 1], -PY),
            (kp.at[0, depth], kp.at[0, 0], PY),
            (kup.at[pl.ds(1, depth)], klow.at[pl.ds(1, depth)], 1),
            (kdn.at[pl.ds(1, depth)], khigh.at[pl.ds(1, depth)], -1),
            (kup.at[1, 0], klow.at[depth + 1, 0], -PY + 1),
            (kdn.at[1, 0], khigh.at[depth + 1, 0], -PY - 1),
            (kup.at[depth, 0], klow.at[0, 0], PY + 1),
            (kdn.at[depth, 0], khigh.at[0, 0], PY - 1),
        )):
            messages.append(remote(src, dst, ksend.at[i], krecv.at[i], offset))
        return messages

    def arrive(messages):
        for message in messages:
            message.wait_recv()

    def begin(messages):
        for message in messages:
            message.start()

    def collide_plane(s, p, values_of, adjust=None):
        for half in range(cells // 128):
            z = slice(half * 128, half * 128 + 128)
            done = collide(values_of(z), rates)
            if adjust is not None:
                done = adjust(done, z)
            for k in range(27):
                c[s, p + 1, k, :, z] = done[k]
                a, b, e = k // 9, k // 3 % 3, k % 3
                if b == 2:
                    yup[s, p + 1, a, e, :, z] = done[k][rows - 1:rows, :]
                elif b == 0:
                    ydn[s, p + 1, a, e, :, z] = done[k][0:1, :]

    def first_collide(p, side=None):
        def adjust(done, z):
            solid = vs[p + 1, 3, :, z] < 0.5
            velocity = [vs[p + 1, d, :, z] for d in range(3)]
            done = list(done)
            for k, c_k in enumerate(VELOCITIES):
                if c_k[0] == side:
                    done[k] = jnp.where(solid, along(velocity, c_k), done[k])
            return done

        collide_plane(0, p, lambda z: [gi[p, k, :, z] for k in range(27)],
                      None if side is None else adjust)

    load_kind.wait()
    load_prof.wait()
    for p in range(1, depth + 1):
        for i in range(2):
            kup[p, i] = kp[i, p, rows - 1:rows, :]
            kdn[p, i] = kp[i, p, 0:1, :]
    def looked_up(profile):
        parts = [jnp.zeros(profile.shape, jnp.float32) for _ in range(3)]
        for i in range(profiles):
            hit = profile == i
            parts = [jnp.where(hit, table[d, i], parts[d]) for d in range(3)]
        return parts

    def source_terms(kind, profile):
        velocity = looked_up(profile)
        opened = (kind == 0) | (kind >= 3)
        vent = kind == 2
        terms = [jnp.where(vent, 6.0 * part, 0.0) for part in velocity]
        return terms + [jnp.where(opened, 1.0, 0.0)], velocity

    load_rates.wait()
    load_table.wait()

    @pl.loop(1, depth + 1)
    def _(pp):
        terms, velocity = source_terms(kp[0, pp], kp[1, pp])
        inflow = kp[0, pp] == 3
        for d in range(4):
            vs[pp, d] = terms[d]
        for d in range(3):
            forced[pp, d] = jnp.where(inflow, velocity[d], 0.0)

    loads[0].wait()
    first_collide(0, -1)
    loads[last].wait()
    first_collide(last, 1)
    for p in range(1, last):
        loads[p].wait()

    @pl.loop(1, last)
    def _(p):
        first_collide(p)

    pl.semaphore_wait(barrier, len(offsets))
    begin(kind_messages())
    begin(y_mid(0) + y_low(0) + y_high(0))
    begin(low_face(0))
    begin(high_face(0))

    for message in kind_messages():
        message.wait_recv()

    for pp in (0, depth + 1):
        kind = kp[0, pp]
        vs[pp, 3] = jnp.where((kind == 0) | (kind >= 3), 1.0, 0.0)
        for rows_in, rows_out in ((klow, vlow), (khigh, vhigh)):
            kind = rows_in[pp, 0]
            rows_out[pp, 3] = jnp.where((kind == 0) | (kind >= 3), 1.0, 0.0)

    @pl.loop(1, depth + 1)
    def _(pp):
        for rows_in, rows_out in ((klow, vlow), (khigh, vhigh)):
            terms, _ = source_terms(rows_in[pp, 0], rows_in[pp, 1])
            for d in range(4):
                rows_out[pp, d] = terms[d]

    def shifted(value, low_row, high_row, b, e):
        if b == 1:
            value = jnp.where(row == 0, low_row(), pltpu.roll(value, 1, 0))
        elif b == -1:
            value = jnp.where(row == rows - 1, high_row(), pltpu.roll(value, rows - 1, 0))
        if e == 1:
            value = pltpu.roll(value, 1, 1)
        elif e == -1:
            value = pltpu.roll(value, cells - 1, 1)
        return value

    place = lax.rem(me + PY // 2, PY)
    below_outside = (row == 0) & (place == 0)
    above_outside = (row == rows - 1) & (place == PY - 1)

    def bounce_plane(p, steps_x):
        for k, (a, b, e) in enumerate(VELOCITIES):
            if a not in steps_x:
                continue
            pp = p + 1 - a
            outer = isinstance(pp, int) and pp in (0, depth + 1)

            def term(ref, sent):
                if outer:
                    total = sent
                else:
                    total = along([ref[pp, d] for d in range(3)], (a, b, e))
                    total = jnp.zeros((1, cells), jnp.float32) if total is None else total
                return jnp.where(ref[pp, 3] > 0.5, BIG, total)

            value = shifted(
                term(vs, c[0, pp, k] if outer else None),
                lambda: term(vlow, ylow[0, pp, a + 1, e + 1] if outer else None),
                lambda: term(vhigh, yhigh[0, pp, a + 1, e + 1] if outer else None), b, e)
            if b == 1:
                value = jnp.where(below_outside, 0.0, value)
            elif b == -1:
                value = jnp.where(above_outside, 0.0, value)
            if e == 1:
                value = jnp.where(lane == 0, 0.0, value)
            elif e == -1:
                value = jnp.where(lane == cells - 1, 0.0, value)
            bounce[p, k] = value

    @pl.loop(1, last)
    def _(p):
        bounce_plane(p, (-1, 0, 1))

    bounce_plane(0, (-1, 0))
    bounce_plane(last, (0, 1))

    def pull_plane(s, p):
        for k, (a, b, e) in enumerate(VELOCITIES):
            pp = p + 1 - a
            value = shifted(
                c[s, pp, k],
                lambda: ylow[s, pp, a + 1, e + 1],
                lambda: yhigh[s, pp, a + 1, e + 1], b, e)
            extra = bounce[p, k]
            ps[k] = jnp.where(extra > 0.5 * BIG, value, c[s, p + 1, 26 - k] + extra)

    def applied(p, z):
        passed = [ps[k, :, z] for k in range(27)]
        kind = kp[0, p + 1, :, z]
        u = flow_velocity(passed)
        outflow = kind == 4
        u = [jnp.where(outflow, u[d], forced[p + 1, d, :, z]) for d in range(3)]
        feq = unit_equilibrium(u)
        fluid = kind == 0
        return [jnp.where(fluid, passed[k], feq[k]) for k in range(27)]

    def update(s, p):
        pull_plane(s, p)
        collide_plane(s + 1, p, lambda z: applied(p, z))

    def finish(s, p):
        pull_plane(s, p)
        for half in range(cells // 128):
            z = slice(half * 128, half * 128 + 128)
            done = applied(p, z)
            for k in range(27):
                out[k, 0, p, :, z] = done[k]

    low = (low_face, y_low, 0, last)
    high = (high_face, y_high, last, 0)
    faces = [low, high]
    for s in range(STEPS):
        arrive(y_low(s) + y_high(s) + y_mid(s))

        @pl.loop(1, last)
        def _(p):
            if s < STEPS - 1:
                update(s, p)
            else:
                finish(s, p)

        if s < STEPS - 1:
            begin(y_mid(s + 1))
        for face in faces:
            arrive(face[0](s))
            p = face[3]
            if s == 0:
                bounce_plane(p, (1,) if p == 0 else (-1,))
            if s < STEPS - 1:
                update(s, p)
                leaves = low if p == 0 else high
                begin(leaves[1](s + 1) + leaves[0](s + 1))
            else:
                finish(s, p)
        faces = faces[::-1]

    for message in kind_messages():
        message.wait_send()
    for s in range(STEPS):
        for message in low_face(s) + high_face(s) + y_low(s) + y_high(s) + y_mid(s):
            message.wait_send()


def solution(mesh):
    n = mesh.shape["gx"]

    def local(populations, cell_kind, profile, vent_table, rates):
        depth, rows, cells = populations.shape[2:]
        profiles = vent_table.shape[0]
        f32, i32 = jnp.float32, jnp.int32
        outer = depth + 2
        vm = pltpu.VMEM
        dma = pltpu.SemaphoreType.DMA

        def body(*refs):
            kernel(n, depth, rows, cells, profiles, *refs)

        return pl.pallas_call(
            body,
            out_shape=pltpu.VMEM(populations.shape, f32),
            in_specs=[
                pl.BlockSpec(memory_space=pl.ANY),
                pl.BlockSpec(memory_space=pl.ANY),
                pl.BlockSpec(memory_space=pl.ANY),
                pl.BlockSpec(memory_space=pl.ANY),
                pl.BlockSpec(memory_space=pl.ANY),
            ],
            out_specs=pl.BlockSpec(memory_space=pltpu.VMEM),
            scratch_shapes=[
                pltpu.SMEM((3, profiles), f32),
                pltpu.SMEM((27,), f32),
                vm((depth, 27, rows, cells), f32),
                vm((2, outer, rows, cells), i32),
                vm((outer, 2, 1, cells), i32),
                vm((outer, 2, 1, cells), i32),
                vm((outer, 2, 1, cells), i32),
                vm((outer, 2, 1, cells), i32),
                vm((outer, 4, rows, cells), f32),
                vm((outer, 4, 1, cells), f32),
                vm((outer, 4, 1, cells), f32),
                vm((outer, 3, rows, cells), f32),
                vm((depth, 27, rows, cells), f32),
                vm((STEPS, outer, 27, rows, cells), f32),
                vm((STEPS, outer, 3, 3, 1, cells), f32),
                vm((STEPS, outer, 3, 3, 1, cells), f32),
                vm((STEPS, outer, 3, 3, 1, cells), f32),
                vm((STEPS, outer, 3, 3, 1, cells), f32),
                vm((27, rows, cells), f32),
                dma((depth + 4,)),
                dma((8,)),
                dma((8,)),
                dma((STEPS, 16)),
                dma((STEPS, 16)),
            ],
            compiler_params=pltpu.CompilerParams(collective_id=0, has_side_effects=True, vmem_limit_bytes=32*1024*1024),
        )(*[pltpu.with_memory_space_constraint(x, pltpu.HBM) for x in (populations, cell_kind, profile, vent_table.T, rates)])

    return jax.shard_map(
        local,
        mesh=mesh,
        in_specs=(
            P("scen", "gx", None, None, None),
            P("gx", None, None, "scen"),
            P("gx", None, None, "scen"),
            P("scen", None),
            P(),
        ),
        out_specs=P("scen", "gx", None, None, None),
        check_vma=False,
    )
```
